16 devices in a mesh: data: 2 (over y, z), dap: 8 (over x, core).
Axes of the slice: x: 4, y: 2, z: 1, core: 2. Of those that a mesh axis runs over, the one named last changes fastest.
The devices are a block of a 4x4x8 slice.
Arguments:
- z_one: bfloat16 [1536, 768, 128], P(('data', 'dap')), parts along dimension 0
- mask_one: int32 [1536, 768], P(('data', 'dap')), parts along dimension 0
- z_two: bfloat16 [1536, 768, 128], P(('data', 'dap')), parts along dimension 0
- mask_two: int32 [1536, 768], P(('data', 'dap')), parts along dimension 0
- norm_in: bfloat16 [2, 2, 128], replicated
- w_proj: bfloat16 [2, 128, 512], replicated
- w_gate: bfloat16 [2, 128, 128], replicated
- norm_mid: bfloat16 [2, 2, 128], replicated
- w_out: bfloat16 [2, 128, 128], replicated
Outputs:
- output 1: bfloat16 [1536, 768, 128], P(('data', 'dap')), parts along dimension 0
- output 2: bfloat16 [1536, 768, 128], P(('data', 'dap')), parts along dimension 0
There are 2 independent parts. The reference program is written for one: setup_inputs(seed, part) draws one part's arguments, and reference() takes and returns one part's arrays. A program takes and returns all parts, laid end to end along the dimension named above; an argument that names none is the same for every part.
All inputs are finite; a program needn't handle non-finite values.
Results may differ from the reference program's by a relative error of at most 0.00447492.
Values are sent between devices in bfloat16 or wider.
A program may use at most 768 MiB of HBM per device.

```python
import jax
import jax.numpy as jnp
from jax import lax

N = 768
CZ = 128
C = 128


def layer_norm(vals, ln_gain, ln_shift):
    vals = vals.astype(jnp.float32)
    row_mean = jnp.mean(vals, axis=-1, keepdims=True)
    centred = vals - row_mean
    row_var = jnp.mean(centred * centred, axis=-1, keepdims=True)
    return centred * lax.rsqrt(row_var + 1e-5) * ln_gain.astype(jnp.float32) + ln_shift.astype(jnp.float32)


def draw_mask(mask_key):
    residue_ok = (jax.random.randint(mask_key, (N,), 0, 20) != 0).astype(jnp.int32)
    return residue_ok[:, None] * residue_ok[None, :]


def setup_inputs(seed: int = 0, part: int = 0) -> dict:
    part_keys = jax.random.split(jax.random.fold_in(jax.random.key(seed), part), 4)
    shared_keys = jax.random.split(jax.random.key(seed + 1), 5)
    norm_base = jnp.array([1.0, 0.0], jnp.float32)[None, :, None]
    return {
        "z_one": jax.random.normal(part_keys[0], (N, N, CZ), jnp.float32).astype(jnp.bfloat16),
        "mask_one": draw_mask(part_keys[1]),
        "z_two": jax.random.normal(part_keys[2], (N, N, CZ), jnp.float32).astype(jnp.bfloat16),
        "mask_two": draw_mask(part_keys[3]),
        "norm_in": (0.3 * jax.random.normal(shared_keys[0], (2, 2, CZ), jnp.float32) + norm_base).astype(jnp.bfloat16),
        "w_proj": (jax.random.normal(shared_keys[1], (2, CZ, 4 * C), jnp.float32) * CZ ** -0.5).astype(jnp.bfloat16),
        "w_gate": (jax.random.normal(shared_keys[2], (2, CZ, CZ), jnp.float32) * CZ ** -0.5).astype(jnp.bfloat16),
        "norm_mid": (0.3 * jax.random.normal(shared_keys[3], (2, 2, C), jnp.float32) + norm_base).astype(jnp.bfloat16),
        "w_out": (jax.random.normal(shared_keys[4], (2, C, CZ), jnp.float32) * C ** -0.5).astype(jnp.bfloat16),
    }


def project_row(z_row, mask_row, norm_in, w_proj):
    x_row = layer_norm(z_row, norm_in[0], norm_in[1]).astype(jnp.bfloat16)
    projected = jnp.dot(x_row, w_proj, preferred_element_type=jnp.float32)
    keep_mask = mask_row.astype(jnp.float32)[:, None]
    a_row = keep_mask * jax.nn.sigmoid(projected[:, C:2 * C]) * projected[:, :C]
    b_row = keep_mask * jax.nn.sigmoid(projected[:, 3 * C:]) * projected[:, 2 * C:3 * C]
    return a_row.astype(jnp.bfloat16), b_row.astype(jnp.bfloat16)


def output_row(z_row, t_row, norm_in, w_gate, norm_mid, w_out):
    x_row = layer_norm(z_row, norm_in[0], norm_in[1]).astype(jnp.bfloat16)
    gate_val = jax.nn.sigmoid(jnp.dot(x_row, w_gate, preferred_element_type=jnp.float32))
    t_norm = layer_norm(t_row, norm_mid[0], norm_mid[1]).astype(jnp.bfloat16)
    update = jnp.dot(t_norm, w_out, preferred_element_type=jnp.float32)
    return (z_row.astype(jnp.float32) + gate_val * update).astype(jnp.bfloat16)


def tri_update(z_pair, pair_mask, norm_in, w_proj, w_gate, norm_mid, w_out, form):
    a_side, b_side = lax.map(lambda row_pair: project_row(row_pair[0], row_pair[1], norm_in, w_proj), (z_pair, pair_mask))
    tri_prod = jnp.einsum(form, a_side.astype(jnp.float32), b_side.astype(jnp.float32)).astype(jnp.bfloat16)
    return lax.map(lambda row_pair: output_row(row_pair[0], row_pair[1], norm_in, w_gate, norm_mid, w_out), (z_pair, tri_prod))


def run_crop(z_pair, pair_mask, norm_in, w_proj, w_gate, norm_mid, w_out):
    z_mid = tri_update(z_pair, pair_mask, norm_in[0], w_proj[0], w_gate[0], norm_mid[0], w_out[0], "ikc,jkc->ijc")
    return tri_update(z_mid, pair_mask, norm_in[1], w_proj[1], w_gate[1], norm_mid[1], w_out[1], "kic,kjc->ijc")


def reference(z_one, mask_one, z_two, mask_two, norm_in, w_proj, w_gate, norm_mid, w_out):
    return (run_crop(z_one, mask_one, norm_in, w_proj, w_gate, norm_mid, w_out),
            run_crop(z_two, mask_two, norm_in, w_proj, w_gate, norm_mid, w_out))
```

```python
import functools

import jax
import jax.numpy as jnp
from jax import lax
from jax.experimental import pallas as pl
from jax.experimental.pallas import tpu as pltpu
from jax.sharding import PartitionSpec as P


F32 = jnp.float32
BF16 = jnp.bfloat16
LANES = 128
ROWS = 16
STRIDE = 20
PAD = 4
AHEAD = 2
EPS = 1e-5
NT = (((1,), (1,)), ((), ()))
TN = (((0,), (0,)), ((), ()))
VMEM_LIMIT = 62 * 2 ** 20
COST = 0.02


def lane_norm(z, gain, shift):
    mean = jnp.mean(z, axis=-1, keepdims=True)
    cent = z - mean
    var = jnp.mean(cent * cent, axis=-1, keepdims=True)
    return (cent * lax.rsqrt(var + EPS) * gain + shift).astype(BF16)


def project_kernel(parts, sides, *refs):
    z_refs, mask_refs = refs[:parts], refs[parts:2 * parts]
    norm_ref, w_ref = refs[2 * parts:2 * parts + 2]
    out_refs, stage, x_ref = refs[2 * parts + 2:-2], refs[-2], refs[-1]
    hidden = w_ref.shape[0] // (2 * sides)
    depth = out_refs[0].shape[2]
    slabs = depth // LANES

    def prepare(i, slot):
        z = jnp.concatenate([r[i] for r in z_refs], axis=0)
        x_ref[slot] = lane_norm(z.astype(F32), norm_ref[0:1, :], norm_ref[1:2, :])

    def row(i, slot):
        keep = jnp.concatenate([r[pl.ds(i, 1), :] for r in mask_refs], axis=1).astype(F32) * 0.5
        q = lax.dot_general(w_ref[...], x_ref[slot], NT, preferred_element_type=F32)
        for side in range(sides):
            base = 2 * hidden * side
            val = (keep * jnp.tanh(q[base + hidden:base + 2 * hidden]) + keep) * q[base:base + hidden]
            for slab in range(slabs):
                stage[side * slabs + slab, pl.ds(i, hidden, stride=STRIDE), :] = val[:, slab * LANES:(slab + 1) * LANES]

    ahead = AHEAD
    for k in range(ahead):
        prepare(k, k)

    def rows_step(g, carry):
        for k in range(ahead):
            row(g * ahead + k, k)
            prepare(jnp.minimum(g * ahead + k + ahead, ROWS - 1), k)
        return carry

    lax.fori_loop(0, ROWS // ahead, rows_step, 0)
    group = 16

    def flush(g, carry):
        for side in range(sides):
            for slab in range(slabs):
                for c in range(group):
                    vals = stage[side * slabs + slab, pl.ds((g * group + c) * STRIDE, ROWS), :].astype(BF16)
                    out_refs[side][g * group + c, :, slab * LANES:(slab + 1) * LANES] = vals
        return carry

    lax.fori_loop(0, hidden // group, flush, 0)


def project(z_parts, mask_parts, norm, w_t, sides):
    rows = z_parts[0].shape[0]
    depths = [z.shape[1] for z in z_parts]
    depth = sum(depths)
    width = z_parts[0].shape[2]
    w_t = w_t[w_t.shape[0] // 2 * (2 - sides):]
    hidden = w_t.shape[0] // (2 * sides)
    gates = jnp.arange(w_t.shape[0]) // hidden % 2 == 1
    w_t = jnp.where(gates[:, None], w_t * 0.5, w_t).astype(BF16)
    whole = lambda x: pl.BlockSpec(x.shape, lambda i: (0,) * x.ndim)
    return pl.pallas_call(
        functools.partial(project_kernel, len(z_parts), sides),
        grid=(rows // ROWS,),
        in_specs=[pl.BlockSpec((ROWS, d, width), lambda i: (i, 0, 0)) for d in depths]
        + [pl.BlockSpec((ROWS, d), lambda i: (i, 0)) for d in depths] + [whole(norm), whole(w_t)],
        out_specs=[pl.BlockSpec((hidden, ROWS, depth), lambda i: (0, i, 0))] * sides,
        out_shape=[jax.ShapeDtypeStruct((hidden, rows, depth), BF16)] * sides,
        scratch_shapes=[pltpu.VMEM((sides * depth // LANES, hidden * STRIDE, LANES), F32),
                        pltpu.VMEM((AHEAD, depth, width), BF16)],
        compiler_params=pltpu.CompilerParams(vmem_limit_bytes=VMEM_LIMIT),
        cost_estimate=pl.CostEstimate(flops=int(COST * 1e9 * (0.4 if sides == 1 else 0.5)), transcendentals=0,
                                      bytes_accessed=rows * depth * (2 * width + 2 * hidden * sides)),
        name="project",
    )(*z_parts, *mask_parts, norm, w_t)


def mix_kernel(pieces, half, n_in, info, *refs):
    a_refs, b_refs = refs[:pieces], refs[pieces:pieces + 2]
    z_ref, norm_ref, mid_ref, w_gate_ref, w_out_ref = refs[pieces + 2:pieces + 7]
    out_ref, acc = refs[n_in:]
    step = pl.program_id(0)
    chunk, rows, _ = a_refs[0].shape
    pitch = rows + PAD
    channels = acc.shape[1] // pitch

    for c in range(chunk):
        a = jnp.concatenate([r[c] for r in a_refs], axis=1) if pieces > 1 else a_refs[0][c]
        for h in range(2):
            if pieces > 1:
                b = jnp.concatenate([r[c, h * half:(h + 1) * half] for r in b_refs], axis=1)
            else:
                b = b_refs[h][c]
            t = lax.dot_general(a, b, NT, preferred_element_type=F32)
            acc[h, pl.ds((step * chunk + c) * pitch, rows), 0:half] = t.astype(BF16).astype(F32)

    @pl.when(step == pl.num_programs(0) - 1)
    def _():
        flip = info[2] if pieces == 1 else 0
        starts = [pl.multiple_of(flip * half, 32), pl.multiple_of((1 - flip) * half, 32)]

        def row(i, carry):
            t = jnp.concatenate([acc[h, pl.ds(i, channels, stride=pitch), :] for h in range(2)], axis=1)
            cent = t - jnp.mean(t, axis=0, keepdims=True)
            var = jnp.mean(cent * cent, axis=0, keepdims=True)
            y = (cent * lax.rsqrt(var + EPS) * mid_ref[0] + mid_ref[1]).astype(BF16)
            update = lax.dot_general(y, w_out_ref[...], TN, preferred_element_type=F32)
            z = jnp.concatenate([z_ref[i, pl.ds(s, half), :] for s in starts], axis=0).astype(F32)
            x = lane_norm(z, norm_ref[0:1, :], norm_ref[1:2, :])
            gate = 0.5 * jnp.tanh(0.5 * jnp.dot(x, w_gate_ref[...], preferred_element_type=F32)) + 0.5
            update = jnp.concatenate([update[0:half], update[LANES:LANES + half]], axis=0)
            new = (z + gate * update).astype(BF16)
            for h, s in enumerate(starts):
                out_ref[i, pl.ds(s, half), :] = new[h * half:(h + 1) * half]
            return carry

        lax.fori_loop(0, rows, row, 0, unroll=4)


def mix(a_parts, b_parts, z, col_block, core, norm, mid, w_gate, w_out, rows, whole=None, dest=None):
    pieces = len(a_parts)
    hidden, _, depth = a_parts[0].shape
    half = b_parts[0].shape[1] // (1 if pieces == 1 else 2)
    cols, width = 2 * half, z.shape[2]
    chunk = 8
    pick = (lambda c, s: (c, 0, 0)) if pieces == 1 else (lambda c, s: (c, s[2], 0))
    zero = jnp.zeros((), jnp.int32)
    info = jnp.stack([col_block, zero if dest is None else dest, core]).astype(jnp.int32)
    mid_wide = jnp.broadcast_to(mid[:, :, None], (*mid.shape, 2 * LANES))
    fixed = lambda x: pl.BlockSpec(x.shape, lambda c, s: (0,) * x.ndim)
    args = [*a_parts, *b_parts, z, norm, mid_wide, w_gate, w_out]
    in_specs = ([pl.BlockSpec((chunk, rows, depth), pick)] * pieces
                + [pl.BlockSpec((chunk, b_parts[0].shape[1], depth), lambda c, s: (c, 0, 0))] * 2
                + [pl.BlockSpec((rows, cols, width), lambda c, s: (0, s[0], 0))] + [fixed(x) for x in args[pieces + 3:]])
    alias = {}
    total = cols if whole is None else whole if isinstance(whole, int) else whole.shape[1]
    if total != cols and not isinstance(whole, int):
        alias = {1 + len(args): 0}
        args.append(whole)
        in_specs.append(pl.BlockSpec(memory_space=pl.ANY))
    return pl.pallas_call(
        functools.partial(mix_kernel, pieces, half, len(args)),
        grid_spec=pltpu.PrefetchScalarGridSpec(
            num_scalar_prefetch=1, grid=(hidden // chunk,), in_specs=in_specs,
            out_specs=pl.BlockSpec((rows, cols, width), lambda c, s: (0, s[1], 0)),
            scratch_shapes=[pltpu.VMEM((2, hidden * (rows + PAD), LANES), F32)]),
        out_shape=jax.ShapeDtypeStruct((rows, total, width), BF16),
        input_output_aliases=alias,
        compiler_params=pltpu.CompilerParams(vmem_limit_bytes=VMEM_LIMIT),
        cost_estimate=pl.CostEstimate(flops=int(COST * 0.45e9), transcendentals=0,
                                      bytes_accessed=2 * hidden * depth * pieces * (rows + cols)),
        name="mix",
    )(info, *args)


def solution(mesh):
    group = mesh.shape["dap"]
    cores = 2
    chips = group // cores

    def shift(x, by):
        return lax.ppermute(x, "dap", [(((c + by) % chips) * cores + s, c * cores + s) for c in range(chips) for s in range(cores)])

    def swap(x):
        return lax.ppermute(x, "dap", [(i, i ^ 1) for i in range(group)])

    def per_device(z_one, mask_one, z_two, mask_two, norm_in, w_proj, w_gate, norm_mid, w_out):
        assert chips == 4
        index = lax.axis_index("dap")
        chip, core = index // cores, index % cores
        hidden = w_out.shape[1]
        rows = z_one.shape[0]
        cols = rows * cores
        zero = jnp.zeros((), jnp.int32)
        turns = (1, -1)
        crops = range(len(turns))
        z0, mask = (z_one, z_two), (mask_one, mask_two)

        def weights(u):
            w = w_proj[u].reshape(w_proj.shape[1], 2, 2, hidden)
            w_t = w.transpose(1, 2, 3, 0).reshape(4 * hidden, -1)
            norm = norm_in[u].astype(F32)
            return (norm, w_t), (norm, norm_mid[u].astype(F32), w_gate[u], w_out[u], rows)

        def at(n, ahead):
            return (chip + turns[n] * ahead) % chips

        def mask_rows(n, ahead):
            return lax.dynamic_slice_in_dim(whole_mask[n], (at(n, ahead) * cores + core) * rows, rows, 0)

        def mask_cols(n, ahead):
            strip = lax.dynamic_slice_in_dim(mask_t[n], at(n, ahead) * cols, cols, 0)
            return [lax.dynamic_slice_in_dim(strip, (at(n, r) * cores + core) * rows, rows, 1) for r in range(chips)]

        turned = lambda x: jnp.swapaxes(x, 0, 1)
        tie = lax.optimization_barrier

        par, fin = weights(0)
        z1 = [shift(z0[n], turns[n]) for n in crops]
        whole_mask = [lax.all_gather(m, "dap", axis=0, tiled=True) for m in mask]
        ab0 = [project([z0[n]], [mask[n]], *par, 2) for n in crops]
        b0s = [swap(ab0[n][1]) for n in crops]
        x00 = [mix([ab0[n][0]], [ab0[n][1], b0s[n]], z0[n], at(n, 0), core, *fin) for n in crops]
        z1, x00, whole_mask = tie((z1, x00, whole_mask))
        z2 = [shift(z1[n], turns[n]) for n in crops]
        ab1 = [project([z1[n]], [mask_rows(n, 1)], *par, 2) for n in crops]
        b1s = [swap(ab1[n][1]) for n in crops]
        x10 = [mix([ab1[n][0]], [ab0[n][1], b0s[n]], z1[n], at(n, 0), core, *fin) for n in crops]
        x01 = [mix([ab0[n][0]], [ab1[n][1], b1s[n]], z0[n], at(n, 1), core, *fin) for n in crops]
        t00, t10, t01 = [[turned(x[n]) for n in crops] for x in (x00, x10, x01)]
        mask_t = [m.T for m in whole_mask]

        first, second = crops
        l1 = [shift(x[first], turns[first]) for x in (t00, t10, t01)]
        r1 = [shift(t01[first], -turns[first])]
        z2, t00, t10, t01 = tie((z2, t00, t10, t01))
        b2, b2s, x02, t02 = [None] * 2, [None] * 2, [None] * 2, [None] * 2
        for n in crops:
            b2[n], = project([z2[n]], [mask_rows(n, 2)], *par, 1)
            b2s[n] = swap(b2[n])
        x02[first] = mix([ab0[first][0]], [b2[first], b2s[first]], z0[first], at(first, 2), core, *fin)
        t02[first], b2[second] = tie((turned(x02[first]), b2[second]))
        r1.append(shift(t02[first], -turns[first]))
        x02[second] = mix([ab0[second][0]], [b2[second], b2s[second]], z0[second], at(second, 2), core, *fin)
        t02[second] = turned(x02[second])

        par, fin = weights(1)

        def columns(n, got):
            t11, t21, t12, t30, t31, t22, t32, t20 = got
            return ([t00[n], t10[n], t20, t30], [t01[n], t11, t21, t31], [t02[n], t12, t22, t32])

        def column(n, k, parts):
            return project(parts, mask_cols(n, k), *par, 1 if k == 2 else 2)

        def both(sides):
            return sides, [swap(s) for s in sides]

        def turn_block(one, two, x, **where):
            (own, other), (own_b, other_b) = one, two
            return mix([own[0], other[0]], [own_b[-1], other_b[-1]], x, zero, core, *fin, **where)

        l1, r1, own = tie((l1, r1, (t00[second], t10[second], t01[second], t02[second])))
        t00[second], t10[second], t01[second], t02[second] = own
        r2 = shift(r1[1], -turns[first])
        l2 = [shift(x, turns[first]) for x in l1[:2]]
        m1 = [shift(x[second], turns[second]) for x in (t00, t10, t01)]
        s1 = [shift(x[second], -turns[second]) for x in (t01, t02)]

        n = first
        col0, col1, col2 = columns(n, (*l1, *r1, *l2, r2))
        c1, col0 = tie((column(n, 1, col1), col0))
        c1 = both(c1)
        c0 = both(column(n, 0, col0))
        y10 = turn_block(c1, c0, x10[n])
        y03 = shift(y10, -turns[n])
        out, y10 = tie((x00[n], y10))
        out = turn_block(c0, c0, out, whole=cols * chips, dest=at(n, 0))
        out = turn_block(c0, c1, x01[n], whole=out, dest=at(n, 1))
        m1, col2, out = tie((m1, col2, out))
        m2 = [shift(x, turns[second]) for x in m1[:2]]
        c2 = both(column(n, 2, col2))
        out = turn_block(c0, c2, x02[n], whole=out, dest=at(n, 2))
        s1, out, m1 = tie((s1, out, m1))
        s2 = shift(s1[1], -turns[second])
        out_one = lax.dynamic_update_slice_in_dim(out, y03, at(n, 3) * cols, 1)

        n = second
        col0, col1, col2 = columns(n, (*m1, *s1, *m2, s2))
        c1, col0 = tie((column(n, 1, col1), col0))
        c1 = both(c1)
        c0, col2 = tie((column(n, 0, col0), col2))
        c0 = both(c0)
        c2, last = tie((column(n, 2, col2), x10[n]))
        c2 = both(c2)
        y10 = turn_block(c1, c0, last)
        y03 = shift(y10, -turns[n])
        out, y10 = tie((x00[n], y10))
        out = turn_block(c0, c0, out, whole=cols * chips, dest=at(n, 0))
        out = turn_block(c0, c1, x01[n], whole=out, dest=at(n, 1))
        out = turn_block(c0, c2, x02[n], whole=out, dest=at(n, 2))
        out_two = lax.dynamic_update_slice_in_dim(out, y03, at(n, 3) * cols, 1)
        return out_one, out_two


    row_spec = P(("data", "dap"), None, None)
    mask_spec = P(("data", "dap"), None)
    return jax.shard_map(per_device, mesh=mesh,
                         in_specs=(row_spec, mask_spec, row_spec, mask_spec, P(), P(), P(), P(), P()),
                         out_specs=(row_spec, row_spec), check_vma=False)
```

```python
import functools

import jax
import jax.numpy as jnp
from jax import lax
from jax.experimental import pallas as pl
from jax.experimental.pallas import tpu as pltpu
from jax.sharding import PartitionSpec as P


F32 = jnp.float32
BF16 = jnp.bfloat16
LANES = 128
ROWS = 16
STRIDE = 20
PAD = 4
AHEAD = 2
EPS = 1e-5
NT = (((1,), (1,)), ((), ()))
TN = (((0,), (0,)), ((), ()))
VMEM_LIMIT = 62 * 2 ** 20
COST = 0.02


def lane_norm(z, gain, shift):
    mean = jnp.mean(z, axis=-1, keepdims=True)
    cent = z - mean
    var = jnp.mean(cent * cent, axis=-1, keepdims=True)
    return (cent * lax.rsqrt(var + EPS) * gain + shift).astype(BF16)


def project_kernel(parts, sides, *refs):
    z_refs, mask_refs = refs[:parts], refs[parts:2 * parts]
    norm_ref, w_ref = refs[2 * parts:2 * parts + 2]
    out_refs, stage, x_ref = refs[2 * parts + 2:-2], refs[-2], refs[-1]
    hidden = w_ref.shape[0] // (2 * sides)
    depth = out_refs[0].shape[2]
    slabs = depth // LANES

    def prepare(i, slot):
        z = jnp.concatenate([r[i] for r in z_refs], axis=0)
        x_ref[slot] = lane_norm(z.astype(F32), norm_ref[0:1, :], norm_ref[1:2, :])

    def row(i, slot):
        keep = jnp.concatenate([r[pl.ds(i, 1), :] for r in mask_refs], axis=1).astype(F32) * 0.5
        q = lax.dot_general(w_ref[...], x_ref[slot], NT, preferred_element_type=F32)
        for side in range(sides):
            base = 2 * hidden * side
            val = (keep * jnp.tanh(q[base + hidden:base + 2 * hidden]) + keep) * q[base:base + hidden]
            for slab in range(slabs):
                stage[side * slabs + slab, pl.ds(i, hidden, stride=STRIDE), :] = val[:, slab * LANES:(slab + 1) * LANES]

    ahead = AHEAD
    for k in range(ahead):
        prepare(k, k)

    def rows_step(g, carry):
        for k in range(ahead):
            row(g * ahead + k, k)
            prepare(jnp.minimum(g * ahead + k + ahead, ROWS - 1), k)
        return carry

    lax.fori_loop(0, ROWS // ahead, rows_step, 0)
    group = 16

    def flush(g, carry):
        for side in range(sides):
            for slab in range(slabs):
                for c in range(group):
                    vals = stage[side * slabs + slab, pl.ds((g * group + c) * STRIDE, ROWS), :].astype(BF16)
                    out_refs[side][g * group + c, :, slab * LANES:(slab + 1) * LANES] = vals
        return carry

    lax.fori_loop(0, hidden // group, flush, 0)


def project(z_parts, mask_parts, norm, w_t, sides):
    rows = z_parts[0].shape[0]
    depths = [z.shape[1] for z in z_parts]
    depth = sum(depths)
    width = z_parts[0].shape[2]
    w_t = w_t[w_t.shape[0] // 2 * (2 - sides):]
    hidden = w_t.shape[0] // (2 * sides)
    gates = jnp.arange(w_t.shape[0]) // hidden % 2 == 1
    w_t = jnp.where(gates[:, None], w_t * 0.5, w_t).astype(BF16)
    whole = lambda x: pl.BlockSpec(x.shape, lambda i: (0,) * x.ndim)
    return pl.pallas_call(
        functools.partial(project_kernel, len(z_parts), sides),
        grid=(rows // ROWS,),
        in_specs=[pl.BlockSpec((ROWS, d, width), lambda i: (i, 0, 0)) for d in depths]
        + [pl.BlockSpec((ROWS, d), lambda i: (i, 0)) for d in depths] + [whole(norm), whole(w_t)],
        out_specs=[pl.BlockSpec((hidden, ROWS, depth), lambda i: (0, i, 0))] * sides,
        out_shape=[jax.ShapeDtypeStruct((hidden, rows, depth), BF16)] * sides,
        scratch_shapes=[pltpu.VMEM((sides * depth // LANES, hidden * STRIDE, LANES), F32),
                        pltpu.VMEM((AHEAD, depth, width), BF16)],
        compiler_params=pltpu.CompilerParams(vmem_limit_bytes=VMEM_LIMIT),
        cost_estimate=pl.CostEstimate(flops=int(COST * 1e9 * (0.4 if sides == 1 else 0.5)), transcendentals=0,
                                      bytes_accessed=rows * depth * (2 * width + 2 * hidden * sides)),
        name="project",
    )(*z_parts, *mask_parts, norm, w_t)


def mix_kernel(pieces, half, n_in, info, *refs):
    a_refs, b_refs = refs[:pieces], refs[pieces:pieces + 2]
    z_ref, norm_ref, mid_ref, w_gate_ref, w_out_ref = refs[pieces + 2:pieces + 7]
    out_ref, acc = refs[n_in:]
    step = pl.program_id(0)
    chunk, rows, _ = a_refs[0].shape
    pitch = rows + PAD
    channels = acc.shape[1] // pitch

    for c in range(chunk):
        a = jnp.concatenate([r[c] for r in a_refs], axis=1) if pieces > 1 else a_refs[0][c]
        for h in range(2):
            if pieces > 1:
                b = jnp.concatenate([r[c, h * half:(h + 1) * half] for r in b_refs], axis=1)
            else:
                b = b_refs[h][c]
            t = lax.dot_general(a, b, NT, preferred_element_type=F32)
            acc[h, pl.ds((step * chunk + c) * pitch, rows), 0:half] = t.astype(BF16).astype(F32)

    @pl.when(step == pl.num_programs(0) - 1)
    def _():
        flip = info[2] if pieces == 1 else 0
        starts = [pl.multiple_of(flip * half, 32), pl.multiple_of((1 - flip) * half, 32)]

        def row(i, carry):
            t = jnp.concatenate([acc[h, pl.ds(i, channels, stride=pitch), :] for h in range(2)], axis=1)
            cent = t - jnp.mean(t, axis=0, keepdims=True)
            var = jnp.mean(cent * cent, axis=0, keepdims=True)
            y = (cent * lax.rsqrt(var + EPS) * mid_ref[0] + mid_ref[1]).astype(BF16)
            update = lax.dot_general(y, w_out_ref[...], TN, preferred_element_type=F32)
            z = jnp.concatenate([z_ref[i, pl.ds(s, half), :] for s in starts], axis=0).astype(F32)
            x = lane_norm(z, norm_ref[0:1, :], norm_ref[1:2, :])
            gate = 0.5 * jnp.tanh(0.5 * jnp.dot(x, w_gate_ref[...], preferred_element_type=F32)) + 0.5
            update = jnp.concatenate([update[0:half], update[LANES:LANES + half]], axis=0)
            new = (z + gate * update).astype(BF16)
            for h, s in enumerate(starts):
                out_ref[i, pl.ds(s, half), :] = new[h * half:(h + 1) * half]
            return carry

        lax.fori_loop(0, rows, row, 0, unroll=4)


def mix(a_parts, b_parts, z, col_block, core, norm, mid, w_gate, w_out, rows, whole=None, dest=None):
    pieces = len(a_parts)
    hidden, _, depth = a_parts[0].shape
    half = b_parts[0].shape[1] // (1 if pieces == 1 else 2)
    cols, width = 2 * half, z.shape[2]
    chunk = 16
    pick = (lambda c, s: (c, 0, 0)) if pieces == 1 else (lambda c, s: (c, s[2], 0))
    zero = jnp.zeros((), jnp.int32)
    info = jnp.stack([col_block, zero if dest is None else dest, core]).astype(jnp.int32)
    mid_wide = jnp.broadcast_to(mid[:, :, None], (*mid.shape, 2 * LANES))
    fixed = lambda x: pl.BlockSpec(x.shape, lambda c, s: (0,) * x.ndim)
    args = [*a_parts, *b_parts, z, norm, mid_wide, w_gate, w_out]
    in_specs = ([pl.BlockSpec((chunk, rows, depth), pick)] * pieces
                + [pl.BlockSpec((chunk, b_parts[0].shape[1], depth), lambda c, s: (c, 0, 0))] * 2
                + [pl.BlockSpec((rows, cols, width), lambda c, s: (0, s[0], 0))] + [fixed(x) for x in args[pieces + 3:]])
    alias = {}
    total = cols if whole is None else whole if isinstance(whole, int) else whole.shape[1]
    if total != cols and not isinstance(whole, int):
        alias = {1 + len(args): 0}
        args.append(whole)
        in_specs.append(pl.BlockSpec(memory_space=pl.ANY))
    return pl.pallas_call(
        functools.partial(mix_kernel, pieces, half, len(args)),
        grid_spec=pltpu.PrefetchScalarGridSpec(
            num_scalar_prefetch=1, grid=(hidden // chunk,), in_specs=in_specs,
            out_specs=pl.BlockSpec((rows, cols, width), lambda c, s: (0, s[1], 0)),
            scratch_shapes=[pltpu.VMEM((2, hidden * (rows + PAD), LANES), F32)]),
        out_shape=jax.ShapeDtypeStruct((rows, total, width), BF16),
        input_output_aliases=alias,
        compiler_params=pltpu.CompilerParams(vmem_limit_bytes=VMEM_LIMIT),
        cost_estimate=pl.CostEstimate(flops=int(COST * 0.45e9), transcendentals=0,
                                      bytes_accessed=2 * hidden * depth * pieces * (rows + cols)),
        name="mix",
    )(info, *args)


def solution(mesh):
    group = mesh.shape["dap"]
    cores = 2
    chips = group // cores

    def shift(x, by):
        return lax.ppermute(x, "dap", [(((c + by) % chips) * cores + s, c * cores + s) for c in range(chips) for s in range(cores)])

    def swap(x):
        return lax.ppermute(x, "dap", [(i, i ^ 1) for i in range(group)])

    def per_device(z_one, mask_one, z_two, mask_two, norm_in, w_proj, w_gate, norm_mid, w_out):
        assert chips == 4
        index = lax.axis_index("dap")
        chip, core = index // cores, index % cores
        hidden = w_out.shape[1]
        rows = z_one.shape[0]
        cols = rows * cores
        zero = jnp.zeros((), jnp.int32)
        turns = (1, -1)
        crops = range(len(turns))
        z0, mask = (z_one, z_two), (mask_one, mask_two)

        def weights(u):
            w = w_proj[u].reshape(w_proj.shape[1], 2, 2, hidden)
            w_t = w.transpose(1, 2, 3, 0).reshape(4 * hidden, -1)
            norm = norm_in[u].astype(F32)
            return (norm, w_t), (norm, norm_mid[u].astype(F32), w_gate[u], w_out[u], rows)

        def at(n, ahead):
            return (chip + turns[n] * ahead) % chips

        def mask_cols(n, ahead):
            return [lax.dynamic_slice_in_dim(masks[n][r], at(n, ahead) * cols, cols, 1).T for r in range(chips)]

        turned = lambda x: jnp.swapaxes(x, 0, 1)
        tie = lax.optimization_barrier

        par, fin = weights(0)
        z1 = [shift(z0[n], turns[n]) for n in crops]
        masks = [[mask[n]] + [shift(mask[n], turns[n] * r) for r in (1, 2, -1)] for n in crops]
        ab0 = [project([z0[n]], [mask[n]], *par, 2) for n in crops]
        b0s = [swap(ab0[n][1]) for n in crops]
        x00 = [mix([ab0[n][0]], [ab0[n][1], b0s[n]], z0[n], at(n, 0), core, *fin) for n in crops]
        z1, x00, masks = tie((z1, x00, masks))
        z2 = [shift(z1[n], turns[n]) for n in crops]
        ab1 = [project([z1[n]], [masks[n][1]], *par, 2) for n in crops]
        b1s = [swap(ab1[n][1]) for n in crops]
        x10 = [mix([ab1[n][0]], [ab0[n][1], b0s[n]], z1[n], at(n, 0), core, *fin) for n in crops]
        x01 = [mix([ab0[n][0]], [ab1[n][1], b1s[n]], z0[n], at(n, 1), core, *fin) for n in crops]
        t00, t10, t01 = [[turned(x[n]) for n in crops] for x in (x00, x10, x01)]

        first, second = crops
        l1 = [shift(x[first], turns[first]) for x in (t00, t10, t01)]
        r1 = [shift(t01[first], -turns[first])]
        z2, t00, t10, t01 = tie((z2, t00, t10, t01))
        b2, b2s, x02, t02 = [None] * 2, [None] * 2, [None] * 2, [None] * 2
        for n in crops:
            b2[n], = project([z2[n]], [masks[n][2]], *par, 1)
            b2s[n] = swap(b2[n])
        x02[first] = mix([ab0[first][0]], [b2[first], b2s[first]], z0[first], at(first, 2), core, *fin)
        t02[first], b2[second] = tie((turned(x02[first]), b2[second]))
        r1.append(shift(t02[first], -turns[first]))
        x02[second] = mix([ab0[second][0]], [b2[second], b2s[second]], z0[second], at(second, 2), core, *fin)
        t02[second] = turned(x02[second])

        par, fin = weights(1)

        def columns(n, got):
            t11, t21, t12, t30, t31, t22, t32, t20 = got
            return ([t00[n], t10[n], t20, t30], [t01[n], t11, t21, t31], [t02[n], t12, t22, t32])

        def column(n, k, parts):
            return project(parts, mask_cols(n, k), *par, 1 if k == 2 else 2)

        def both(sides):
            return sides, [swap(s) for s in sides]

        def turn_block(one, two, x, **where):
            (own, other), (own_b, other_b) = one, two
            return mix([own[0], other[0]], [own_b[-1], other_b[-1]], x, zero, core, *fin, **where)

        l1[:2], r1, x02[second] = tie((l1[:2], r1, x02[second]))
        r2 = shift(r1[1], -turns[first])
        l2 = [shift(x, turns[first]) for x in l1[:2]]
        m1 = [shift(x[second], turns[second]) for x in (t00, t10, t01)]
        s1 = [shift(x[second], -turns[second]) for x in (t01, t02)]

        n = first
        col0, col1, col2 = columns(n, (*l1, *r1, *l2, r2))
        c1, col0 = tie((column(n, 1, col1), col0))
        c1 = both(c1)
        c0 = both(column(n, 0, col0))
        y10 = turn_block(c1, c0, x10[n])
        y03 = shift(y10, -turns[n])
        out, y10 = tie((x00[n], y10))
        out = turn_block(c0, c0, out, whole=cols * chips, dest=at(n, 0))
        out = turn_block(c0, c1, x01[n], whole=out, dest=at(n, 1))
        col2, out = tie((col2, out))
        c2 = both(column(n, 2, col2))
        m1, out = tie((m1, out))
        m2 = [shift(x, turns[second]) for x in m1[:2]]
        out = turn_block(c0, c2, x02[n], whole=out, dest=at(n, 2))
        s1, out, m1 = tie((s1, out, m1))
        s2 = shift(s1[1], -turns[second])
        out_one = lax.dynamic_update_slice_in_dim(out, y03, at(n, 3) * cols, 1)

        n = second
        col0, col1, col2 = columns(n, (*m1, *s1, *m2, s2))
        c1, col0 = tie((column(n, 1, col1), col0))
        c1 = both(c1)
        c0, col2 = tie((column(n, 0, col0), col2))
        c0 = both(c0)
        c2, last = tie((column(n, 2, col2), x10[n]))
        c2 = both(c2)
        y10 = turn_block(c1, c0, last)
        y03 = shift(y10, -turns[n])
        out, y10 = tie((x00[n], y10))
        out = turn_block(c0, c0, out, whole=cols * chips, dest=at(n, 0))
        out = turn_block(c0, c1, x01[n], whole=out, dest=at(n, 1))
        out = turn_block(c0, c2, x02[n], whole=out, dest=at(n, 2))
        out_two = lax.dynamic_update_slice_in_dim(out, y03, at(n, 3) * cols, 1)
        return out_one, out_two


    row_spec = P(("data", "dap"), None, None)
    mask_spec = P(("data", "dap"), None)
    return jax.shard_map(per_device, mesh=mesh,
                         in_specs=(row_spec, mask_spec, row_spec, mask_spec, P(), P(), P(), P(), P()),
                         out_specs=(row_spec, row_spec), check_vma=False)
```
